32 devices in a mesh: owner: 4 (over y, core), rows: 8 (over z, x).
Axes of the slice: x: 2, y: 2, z: 4, core: 2. Of those that a mesh axis runs over, the one named last changes fastest.
Arguments:
- w_gate: float32 [128, 2048, 768], P('owner', 'rows'), may hold values from -0.125 to 0.125
- w_up: float32 [128, 2048, 768], P('owner', 'rows'), may hold values from -0.125 to 0.125
- router_weight: float32 [2048, 128], P('rows', 'owner'), may hold values from -0.125 to 0.125
- router_gain: float32 [2048], P('rows'), may hold values from 0.25 to 1.75
Outputs:
- serve_gate: bfloat16 [128, 768, 2048], P('owner', 'rows')
- serve_up: bfloat16 [128, 768, 2048], P('owner', 'rows')
- serve_router: bfloat16 [2048, 128], replicated
The draws below stay inside these ranges and needn't reach their ends.
All inputs are finite; a program needn't handle non-finite values.
Results may differ from the reference program's by a relative error of at most 0.001.
Values may be sent and summed in bfloat16 or wider, within the bound.
A program may use at most 192 MiB of HBM per device.

```python
import jax
import jax.numpy as jnp

EXPERTS = 128
D_MODEL = 2048
D_EXPERT = 768


def steps_of(own_key, extent, pieces, smallest, high):
    factor_of, own = 1.0, jax.random.fold_in(own_key, 6)
    for position, blocks in pieces:
        draws = jnp.exp(jax.random.uniform(jax.random.fold_in(own, position), (blocks,), jnp.float32, smallest / len(pieces), high / len(pieces)))
        factor_of = factor_of * jnp.repeat(draws, extent[position] // blocks).reshape([-1 if axis == position else 1 for axis in range(len(extent))])
    return factor_of


def gaussian(own_key, dims, spread, most, pieces=(), held_as=jnp.bfloat16):
    entries = jax.random.normal(own_key, dims, jnp.float32) * spread
    if len(pieces) > 0:
        entries = steps_of(own_key, dims, pieces, -0.22, 0.18) * entries
    return jnp.clip(entries, min=-most, max=most).astype(held_as)


def setup_inputs(seed: int = 0) -> dict:
    seeds = jax.random.split(jax.random.key(seed), 5)
    return {
        "w_gate": gaussian(seeds[0], (EXPERTS, D_MODEL, D_EXPERT), D_MODEL ** -0.5, 0.125, ((0, 4), (1, 8)), jnp.float32),
        "w_up": gaussian(seeds[1], (EXPERTS, D_MODEL, D_EXPERT), D_MODEL ** -0.5, 0.125, ((0, 4), (1, 8)), jnp.float32),
        "router_weight": gaussian(seeds[2], (D_MODEL, EXPERTS), D_MODEL ** -0.5, 0.125, ((0, 8), (1, 4)), jnp.float32),
        "router_gain": jnp.clip(1.0 + 0.15 * jax.random.normal(seeds[3], (D_MODEL,), jnp.float32), 0.25, 1.75),
    }


def reference(w_gate, w_up, router_weight, router_gain):
    serve_gate = w_gate.astype(jnp.bfloat16)
    serve_gate = jnp.transpose(serve_gate, (0, 2, 1))
    serve_up = w_up.astype(jnp.bfloat16)
    serve_up = jnp.transpose(serve_up, (0, 2, 1))
    serve_router = (router_weight * router_gain[:, None]).astype(jnp.bfloat16)
    return serve_gate, serve_up, serve_router
```

```python
import functools

import jax
import jax.numpy as jnp
from jax import lax
from jax.experimental import pallas as pl
from jax.experimental.pallas import tpu as pltpu
from jax.sharding import PartitionSpec as P

MESH = pl.DeviceIdType.MESH
SLOTS = 4


def flipped(me, k):
    out, bit = me, 1
    while bit <= k:
        if k & bit:
            out = out + bit * (1 - 2 * ((me // bit) % 2))
        bit *= 2
    return out


def exchange(rows, owners, gate_ref, up_ref, router_ref, sgate_ref, sup_ref, srouter_ref,
             taken, turned, read_sem, send_sem, recv_sem, keep_sem, rsend, rrecv, osend, orecv, rkeep):
    me, mine = lax.axis_index("rows"), lax.axis_index("owner")
    experts, depth, width = gate_ref.shape
    part = width // rows
    share = router_ref.shape[0]
    sources, results = (gate_ref, up_ref), (sgate_ref, sup_ref)
    half = rows // 2
    quarter = (me * 4) // rows
    outer = (quarter == 0) | (quarter == 3)

    barrier = pltpu.get_barrier_semaphore()
    for k in range(1, rows):
        pl.semaphore_signal(barrier, inc=1, device_id={"rows": flipped(me, k)}, device_id_type=MESH)
    for k in range(1, owners):
        pl.semaphore_signal(barrier, inc=1, device_id={"owner": lax.rem(mine + k, owners)}, device_id_type=MESH)

    def reading(b, e, m):
        return pltpu.make_async_copy(sources[m].at[e], taken.at[b], read_sem.at[b])

    def place(d, size):
        return pl.ds(pl.multiple_of(d * size, size), size)

    def sending(m, k, which):
        there = flipped(me, k)
        return pltpu.make_async_remote_copy(
            src_ref=turned.at[m, which, place(there, part), :],
            dst_ref=results[m].at[which, :, place(me, depth)],
            send_sem=send_sem.at[m, k],
            recv_sem=recv_sem.at[m, k],
            device_id={"rows": there},
            device_id_type=MESH,
        )

    def router_rows(k):
        return pltpu.make_async_remote_copy(
            src_ref=router_ref,
            dst_ref=srouter_ref.at[place(mine, share), place(me, depth)],
            send_sem=rsend.at[k], recv_sem=rrecv.at[k],
            device_id={"rows": flipped(me, k)}, device_id_type=MESH,
        )

    def router_owner(k):
        return pltpu.make_async_remote_copy(
            src_ref=srouter_ref.at[place(mine, share), :],
            dst_ref=srouter_ref.at[place(mine, share), :],
            send_sem=osend.at[k], recv_sem=orecv.at[k],
            device_id={"owner": lax.rem(mine + k, owners)}, device_id_type=MESH,
        )

    router_keep = pltpu.make_async_copy(
        router_ref, srouter_ref.at[place(mine, share), place(me, depth)], rkeep)

    for b in range(SLOTS):
        reading(b, b // 2, b % 2).start()
    pl.semaphore_wait(barrier, rows - 1 + owners - 1)
    router_keep.start()
    for k in range(1, rows):
        router_rows(k).start()

    far = [k for k in range(rows - 1, half - 1, -1)]
    near = [k for k in range(half - 1, 0, -1)]

    def send_block(e, m):
        @pl.when(jnp.logical_not(outer))
        def _():
            for k in far:
                sending(m, k, pl.ds(e, 1)).start()
        for k in near:
            sending(m, k, pl.ds(e, 1)).start()

    def turn(b, e, m):
        reading(b, e, m).wait()
        for j in range(width // 128):
            block = taken[b, :, j * 128:(j + 1) * 128].astype(jnp.bfloat16)
            turned[m, e, j * 128:(j + 1) * 128, :] = block.T

    per = SLOTS // 2

    def step(i, carry):
        for q in range(per):
            for m in range(2):
                e, b = i * per + q, q * 2 + m
                turn(b, e, m)

                @pl.when(e + per < experts)
                def _():
                    reading(b, e + per, m).start()
            for m in range(2):
                send_block(i * per + q, m)
        return carry

    lax.fori_loop(0, experts // per, step, 0)

    every = pl.ds(0, experts)

    @pl.when(outer)
    def _():
        for m in range(2):
            for k in far:
                sending(m, k, every).start()

    keeps = [pltpu.make_async_copy(
        turned.at[m, :, place(me, part), :], results[m].at[:, :, place(me, depth)], keep_sem.at[m])
        for m in range(2)]
    for copy in keeps:
        copy.start()
    router_keep.wait()
    for k in range(1, rows):
        router_rows(k).wait()
    for k in range(1, owners):
        router_owner(k).start()
    for k in range(1, owners):
        router_owner(k).wait()
    for copy in keeps:
        copy.wait()
    for m in range(2):
        for k in range(1, rows):
            sending(m, k, every).wait()


def fused(rows, owners, w_gate, w_up, router_weight, router_gain):
    experts, depth, width = w_gate.shape
    share = router_weight.shape[1]
    part_router = (router_weight * router_gain[:, None]).astype(jnp.bfloat16).T
    out = jax.ShapeDtypeStruct((experts, width // rows, depth * rows), jnp.bfloat16)
    sems = pltpu.SemaphoreType.DMA
    sent = 2 * experts * depth * width * 2
    serve_gate, serve_up, router = pl.pallas_call(
        functools.partial(exchange, rows, owners),
        out_shape=(out, out, jax.ShapeDtypeStruct((share * owners, depth * rows), jnp.bfloat16)),
        in_specs=[pl.BlockSpec(memory_space=pl.ANY)] * 2 + [pl.BlockSpec(memory_space=pltpu.VMEM)],
        out_specs=[pl.BlockSpec(memory_space=pl.ANY)] * 3,
        scratch_shapes=[
            pltpu.VMEM((SLOTS, depth, width), jnp.float32),
            pltpu.VMEM((2, experts, width, depth), jnp.bfloat16),
            sems((SLOTS,)),
            sems((2, rows)),
            sems((2, rows)),
            sems((2,)),
            sems((rows,)),
            sems((rows,)),
            sems((owners,)),
            sems((owners,)),
            sems,
        ],
        compiler_params=pltpu.CompilerParams(
            collective_id=0, has_side_effects=True, vmem_limit_bytes=60 * 1024 * 1024),
        cost_estimate=pl.CostEstimate(flops=0, bytes_accessed=4 * sent, transcendentals=0),
    )(w_gate, w_up, part_router)
    return serve_gate, serve_up, router.T


def plain(w_gate, w_up, router_weight, router_gain):
    narrow_gate, narrow_up = (w_gate.astype(jnp.bfloat16), w_up.astype(jnp.bfloat16))
    serve_gate, serve_up = (
        lax.all_to_all(narrow_gate, "rows", split_axis=2, concat_axis=1, tiled=True),
        lax.all_to_all(narrow_up, "rows", split_axis=2, concat_axis=1, tiled=True),
    )
    serve_gate = jnp.transpose(serve_gate, (0, 2, 1))
    serve_up = jnp.transpose(serve_up, (0, 2, 1))
    part_router = (router_weight * router_gain[:, None]).astype(jnp.bfloat16)
    row_router = lax.all_gather(part_router, "rows", axis=0, tiled=True)
    serve_router = lax.all_gather(row_router, "owner", axis=1, tiled=True)
    return (serve_gate, serve_up, serve_router)


def solution(mesh):
    rows, owners = mesh.shape["rows"], mesh.shape["owner"]

    def body(w_gate, w_up, router_weight, router_gain):
        experts, depth, width = w_gate.shape
        share = router_weight.shape[1]
        aligned = (
            depth % 128 == 0 and width % 128 == 0 and width % (16 * rows) == 0
            and share % 16 == 0 and experts % (SLOTS // 2) == 0
            and rows >= 4 and rows & (rows - 1) == 0
            and 2 * experts * depth * width * 2 + SLOTS * depth * width * 4 <= 56 * 1024 * 1024
        )
        if aligned:
            return fused(rows, owners, w_gate, w_up, router_weight, router_gain)
        return plain(w_gate, w_up, router_weight, router_gain)

    placed = (P("owner", "rows", None), P("owner", "rows", None), P("rows", "owner"), P("rows"))
    return jax.shard_map(
        body,
        mesh=mesh,
        in_specs=placed,
        out_specs=(P("owner", "rows", None), P("owner", "rows", None), P()),
        check_vma=False,
    )
```

```python
import functools

import jax
import jax.numpy as jnp
from jax import lax
from jax.experimental import pallas as pl
from jax.experimental.pallas import tpu as pltpu
from jax.sharding import PartitionSpec as P

MESH = pl.DeviceIdType.MESH
SLOTS = 4


def flipped(me, k):
    out, bit = me, 1
    while bit <= k:
        if k & bit:
            out = out + bit * (1 - 2 * ((me // bit) % 2))
        bit *= 2
    return out


def exchange(rows, owners, gate_ref, up_ref, weight_ref, gain_ref, sgate_ref, sup_ref, srouter_ref,
             router_ref, taken, turned, read_sem, send_sem, recv_sem, keep_sem, rsend, rrecv, osend, orecv, rkeep):
    me, mine = lax.axis_index("rows"), lax.axis_index("owner")
    experts, depth, width = gate_ref.shape
    part = width // rows
    share = weight_ref.shape[0]
    sources, results = (gate_ref, up_ref), (sgate_ref, sup_ref)
    half = rows // 2
    quarter = (me * 4) // rows
    outer = (quarter == 0) | (quarter == 3)

    barrier = pltpu.get_barrier_semaphore()
    for k in range(1, rows):
        pl.semaphore_signal(barrier, inc=1, device_id={"rows": flipped(me, k)}, device_id_type=MESH)
    for k in range(1, owners):
        pl.semaphore_signal(barrier, inc=1, device_id={"owner": lax.rem(mine + k, owners)}, device_id_type=MESH)

    def reading(b, e, m):
        return pltpu.make_async_copy(sources[m].at[e], taken.at[b], read_sem.at[b])

    def place(d, size):
        return pl.ds(pl.multiple_of(d * size, size), size)

    def sending(m, k, which):
        there = flipped(me, k)
        return pltpu.make_async_remote_copy(
            src_ref=turned.at[m, which, place(there, part), :],
            dst_ref=results[m].at[which, :, place(me, depth)],
            send_sem=send_sem.at[m, k],
            recv_sem=recv_sem.at[m, k],
            device_id={"rows": there},
            device_id_type=MESH,
        )

    def router_rows(k):
        return pltpu.make_async_remote_copy(
            src_ref=router_ref,
            dst_ref=srouter_ref.at[place(mine, share), place(me, depth)],
            send_sem=rsend.at[k], recv_sem=rrecv.at[k],
            device_id={"rows": flipped(me, k)}, device_id_type=MESH,
        )

    def router_owner(k):
        return pltpu.make_async_remote_copy(
            src_ref=srouter_ref.at[place(mine, share), :],
            dst_ref=srouter_ref.at[place(mine, share), :],
            send_sem=osend.at[k], recv_sem=orecv.at[k],
            device_id={"owner": lax.rem(mine + k, owners)}, device_id_type=MESH,
        )

    router_keep = pltpu.make_async_copy(
        router_ref, srouter_ref.at[place(mine, share), place(me, depth)], rkeep)

    for b in range(SLOTS):
        reading(b, b // 2, b % 2).start()
    router_ref[...] = (weight_ref[...] * gain_ref[...]).astype(jnp.bfloat16)
    pl.semaphore_wait(barrier, rows - 1 + owners - 1)
    far = [k for k in range(rows - 1, half - 1, -1)]
    near = [k for k in range(half - 1, 0, -1)]

    def send_block(e, m):
        @pl.when(jnp.logical_not(outer))
        def _():
            for k in far:
                sending(m, k, pl.ds(e, 1)).start()
        for k in near:
            sending(m, k, pl.ds(e, 1)).start()

    def turn(b, e, m):
        reading(b, e, m).wait()
        for j in range(width // 128):
            block = taken[b, :, j * 128:(j + 1) * 128].astype(jnp.bfloat16)
            turned[m, e, j * 128:(j + 1) * 128, :] = block.T

    def advance(b, e, m):
        turn(b, e, m)

        @pl.when(e + per < experts)
        def _():
            reading(b, e + per, m).start()

    per = SLOTS // 2
    advance(0, 0, 0)
    advance(1, 0, 1)
    send_block(0, 0)
    router_keep.start()
    for k in range(1, rows):
        router_rows(k).start()

    def step(e, carry):
        for m in range(2):
            advance(2 * lax.rem(e, per) + m, e, m)
            send_block(e - 1 + m, 1 - m)
        return carry

    lax.fori_loop(1, experts, step, 0)
    send_block(experts - 1, 1)

    every = pl.ds(0, experts)

    @pl.when(outer)
    def _():
        for m in range(2):
            for k in far:
                sending(m, k, every).start()

    keeps = [pltpu.make_async_copy(
        turned.at[m, :, place(me, part), :], results[m].at[:, :, place(me, depth)], keep_sem.at[m])
        for m in range(2)]
    for copy in keeps:
        copy.start()
    router_keep.wait()
    for k in range(1, rows):
        router_rows(k).wait()
    for k in range(1, owners):
        router_owner(k).start()
    for k in range(1, owners):
        router_owner(k).wait()
    for copy in keeps:
        copy.wait()
    for m in range(2):
        for k in range(1, rows):
            sending(m, k, every).wait()


def fused(rows, owners, w_gate, w_up, router_weight, router_gain):
    experts, depth, width = w_gate.shape
    share = router_weight.shape[1]
    out = jax.ShapeDtypeStruct((experts, width // rows, depth * rows), jnp.bfloat16)
    sems = pltpu.SemaphoreType.DMA
    sent = 2 * experts * depth * width * 2
    serve_gate, serve_up, router = pl.pallas_call(
        functools.partial(exchange, rows, owners),
        out_shape=(out, out, jax.ShapeDtypeStruct((share * owners, depth * rows), jnp.bfloat16)),
        in_specs=[pl.BlockSpec(memory_space=pl.ANY)] * 2 + [pl.BlockSpec(memory_space=pltpu.VMEM)] * 2,
        out_specs=[pl.BlockSpec(memory_space=pl.ANY)] * 3,
        scratch_shapes=[
            pltpu.VMEM((share, depth), jnp.bfloat16),
            pltpu.VMEM((SLOTS, depth, width), jnp.float32),
            pltpu.VMEM((2, experts, width, depth), jnp.bfloat16),
            sems((SLOTS,)),
            sems((2, rows)),
            sems((2, rows)),
            sems((2,)),
            sems((rows,)),
            sems((rows,)),
            sems((owners,)),
            sems((owners,)),
            sems,
        ],
        compiler_params=pltpu.CompilerParams(
            collective_id=0, has_side_effects=True, vmem_limit_bytes=60 * 1024 * 1024),
        cost_estimate=pl.CostEstimate(flops=0, bytes_accessed=4 * sent, transcendentals=0),
    )(w_gate, w_up, router_weight.T, router_gain[None, :])
    return serve_gate, serve_up, router.T


def plain(w_gate, w_up, router_weight, router_gain):
    narrow_gate, narrow_up = (w_gate.astype(jnp.bfloat16), w_up.astype(jnp.bfloat16))
    serve_gate, serve_up = (
        lax.all_to_all(narrow_gate, "rows", split_axis=2, concat_axis=1, tiled=True),
        lax.all_to_all(narrow_up, "rows", split_axis=2, concat_axis=1, tiled=True),
    )
    serve_gate = jnp.transpose(serve_gate, (0, 2, 1))
    serve_up = jnp.transpose(serve_up, (0, 2, 1))
    part_router = (router_weight * router_gain[:, None]).astype(jnp.bfloat16)
    row_router = lax.all_gather(part_router, "rows", axis=0, tiled=True)
    serve_router = lax.all_gather(row_router, "owner", axis=1, tiled=True)
    return (serve_gate, serve_up, serve_router)


def solution(mesh):
    rows, owners = mesh.shape["rows"], mesh.shape["owner"]

    def body(w_gate, w_up, router_weight, router_gain):
        experts, depth, width = w_gate.shape
        share = router_weight.shape[1]
        aligned = (
            depth % 128 == 0 and width % 128 == 0 and width % (16 * rows) == 0
            and share % 16 == 0 and experts % (SLOTS // 2) == 0
            and rows >= 4 and rows & (rows - 1) == 0
            and 2 * experts * depth * width * 2 + SLOTS * depth * width * 4 <= 56 * 1024 * 1024
        )
        if aligned:
            return fused(rows, owners, w_gate, w_up, router_weight, router_gain)
        return plain(w_gate, w_up, router_weight, router_gain)

    placed = (P("owner", "rows", None), P("owner", "rows", None), P("rows", "owner"), P("rows"))
    return jax.shard_map(
        body,
        mesh=mesh,
        in_specs=placed,
        out_specs=(P("owner", "rows", None), P("owner", "rows", None), P()),
        check_vma=False,
    )
```
